32 devices in a mesh: fsdp: 2 (over x), ctx: 16 (over z, y, core).
Axes of the slice: x: 2, y: 2, z: 4, core: 2. Of those that a mesh axis runs over, the one named last changes fastest.
Arguments:
- block_input: float32 [2, 2048, 1600], P('fsdp', 'ctx'), may hold values from -6 to 6
- attn_weight: bfloat16 [1600, 6400], P(None, ('fsdp', 'ctx')), may hold values from -4 to 4
- fc_weight: bfloat16 [1600, 6400], P(None, ('fsdp', 'ctx')), may hold values from -0.15625 to 0.15625
- down_weight: bfloat16 [1600, 6400], P(None, ('fsdp', 'ctx')), may hold values from -0.078125 to 0.078125
- vectors: bfloat16 [19200], P(('fsdp', 'ctx')), may hold values from -2.5 to 2
- cotangent: float32 [2, 2048, 1600], P('fsdp', 'ctx'), may hold values from -6 to 6
Outputs:
- block_output: float32 [2, 2048, 1600], P('fsdp', 'ctx')
- input_grad: float32 [2, 2048, 1600], P('fsdp', 'ctx')
- attn_grad: float32 [1600, 6400], P(None, ('fsdp', 'ctx'))
- fc_grad: float32 [1600, 6400], P(None, ('fsdp', 'ctx'))
- down_grad: float32 [1600, 6400], P(None, ('fsdp', 'ctx'))
- vector_grad: float32 [19200], P(('fsdp', 'ctx'))
The draws below stay inside these ranges and needn't reach their ends.
All inputs are finite; a program needn't handle non-finite values.
Results may differ from the reference program's by a relative error of at most 0.01.
Values may be sent and summed in bfloat16 or wider, within the bound.
A program may use at most 512 MiB of HBM per device.

```python
import math
import jax
import jax.numpy as jnp
from jax import lax

D = 1600
HEADS = 25
HEAD_DIM = 64
FF = 6400
SEQ_LEN = 2048
SEQS = 2


def draw_block_input(key, part):
    shape = (SEQS, SEQ_LEN, D)
    return jnp.clip(jax.random.normal(key, shape, jnp.float32), -6.0, 6.0)


def draw_attn_weight(key, part):
    key_main = jax.random.fold_in(key, 0)
    column = jnp.arange(4 * D)
    column_scale = jnp.where(column < 2 * D, 1.2, jnp.where(column < 3 * D, 1.0, 4.0)) * D ** (-0.5)
    weights = jax.random.normal(key_main, (D, 4 * D), jnp.float32) * column_scale[None, :]
    return jnp.clip(weights, -4.0, 4.0).astype(jnp.bfloat16)


def draw_vectors(key, part):
    key_gain, key_bias = jax.random.split(key)
    index_all = jnp.arange(12 * D)
    block_of = index_all // D
    is_gain = (block_of == 0) | (block_of == 5)
    is_up = index_all >= 8 * D
    gains = jax.random.uniform(key_gain, (12 * D,), jnp.float32, 0.7, 1.3)
    biases = jnp.clip(0.3 * jax.random.normal(key_bias, (12 * D,), jnp.float32), -1.5, 1.5)
    biases = jnp.where(is_up, 1.6 * biases, biases)
    return jnp.where(is_gain, gains, biases).astype(jnp.bfloat16)


def levels(own_key, dims, pieces, smallest, high):
    def one(dim, shards_of):
        heights = jax.random.uniform(jax.random.fold_in(jax.random.fold_in(own_key, 6), dim), (shards_of,), jnp.float32, smallest / len(pieces), high / len(pieces))
        return jnp.repeat(jnp.exp(heights), dims[dim] // shards_of).reshape((-1,) + (1,) * (len(dims) - dim - 1))

    gain = one(*pieces[0])
    for cut in pieces[1:]:
        gain = gain * one(*cut)
    return gain


def scatter_about(key, shape, scale, most, pieces=(), held_as=jnp.bfloat16):
    factor_of = levels(key, shape, pieces, -0.22, 0.18) if pieces else 1.0
    result = jax.random.normal(key, shape, jnp.float32) * scale * factor_of
    return jnp.minimum(jnp.maximum(result, -most), most).astype(held_as)


def setup_inputs(seed: int = 0) -> dict:
    splits = jax.random.split(jax.random.key(seed), 7)
    block_input = draw_block_input(jax.random.fold_in(splits[6], 71), 0)
    attn_weight = draw_attn_weight(jax.random.fold_in(splits[6], 71), 0)
    fc_weight = scatter_about(splits[2], (D, FF), D ** -0.5, 0.15625, ((1, 32),))
    down_weight = scatter_about(splits[3], (D, FF), FF ** -0.5, 0.078125, ((1, 32),))
    vectors = draw_vectors(jax.random.fold_in(splits[6], 71), 0)
    cotangent = scatter_about(splits[5], (SEQS, SEQ_LEN, D), 1.0, 6.0, ((0, 2), (1, 16)), jnp.float32)
    return {"block_input": block_input, "attn_weight": attn_weight, "fc_weight": fc_weight, "down_weight": down_weight, "vectors": vectors, "cotangent": cotangent}


epsilon = 1e-05
gelu_coeff = 0.7978845608028654

def layer_norm(values, gain_vec, shift_vec):
    center = values - lax.optimization_barrier(jnp.mean(values, axis=-1, keepdims=True))
    spread = lax.optimization_barrier(jnp.mean(center * center, axis=-1, keepdims=True))
    return center * lax.rsqrt(spread + epsilon) * gain_vec + shift_vec

def gelu_tanh(values):
    return 0.5 * values * (1.0 + jnp.tanh(gelu_coeff * (values + 0.044715 * values * values * values)))

def round_trip(values):
    return lax.optimization_barrier(values.astype(jnp.bfloat16)).astype(jnp.float32)

def reference(block_input, attn_weight, fc_weight, down_weight, vectors, cotangent):
    seq_count = block_input.shape[0]
    length = block_input.shape[1]
    q_rows = math.gcd(length, 128)
    t_rows = math.gcd(length, 4096)
    score_scale = 1.0 / math.sqrt(HEAD_DIM)
    vec_full = vectors.astype(jnp.float32)
    gain_one = vec_full[0:D]
    shift_one = vec_full[D:2 * D]
    bias_query = vec_full[2 * D:3 * D]
    bias_value = vec_full[3 * D:4 * D]
    bias_out = vec_full[4 * D:5 * D]
    gain_two = vec_full[5 * D:6 * D]
    shift_two = vec_full[6 * D:7 * D]
    bias_proj = vec_full[7 * D:8 * D]
    fc_bias = vec_full[8 * D:12 * D]
    w_qkv = attn_weight[:, 0:3 * D]
    w_out = attn_weight[:, 3 * D:4 * D]
    positions = jnp.arange(length, dtype=jnp.int32)
    grad_qkv = jnp.zeros((D, 3 * D), jnp.float32)
    grad_out_proj = jnp.zeros((D, D), jnp.float32)
    mlp_totals = (jnp.zeros((D, FF), jnp.float32), jnp.zeros((D, FF), jnp.float32), jnp.zeros((D,), jnp.float32), jnp.zeros((D,), jnp.float32), jnp.zeros((FF,), jnp.float32), jnp.zeros((D,), jnp.float32))
    vec_totals = [jnp.zeros((D,), jnp.float32) for member in range(5)]
    outputs_list = []
    grads_list = []
    for seq_index in range(seq_count):
        inputs = block_input[seq_index]
        grad_output = cotangent[seq_index]
        normed_one, pull_one = jax.vjp(layer_norm, inputs, gain_one, shift_one)
        normed_low = normed_one.astype(jnp.bfloat16)
        projected = jnp.dot(normed_low, w_qkv, preferred_element_type=jnp.float32)
        queries = round_trip(projected[:, 0:D] + bias_query).reshape(length, HEADS, HEAD_DIM)
        keys = round_trip(projected[:, D:2 * D]).reshape(length, HEADS, HEAD_DIM)
        values = round_trip(projected[:, 2 * D:3 * D] + bias_value).reshape(length, HEADS, HEAD_DIM)

        def forward_block(unused, block_index):
            offset = block_index * q_rows
            query_blk = lax.dynamic_slice_in_dim(queries, offset, q_rows, 0)
            scores = jnp.einsum('qhd,khd->hqk', query_blk, keys) * score_scale
            allowed = positions[None, :] <= (offset + jnp.arange(q_rows, dtype=jnp.int32))[:, None]
            scores = jnp.where(allowed[None], scores, -jnp.inf)
            row_max = lax.optimization_barrier(jnp.max(scores, axis=-1, keepdims=True))
            weights = jnp.exp(scores - row_max)
            row_total = lax.optimization_barrier(jnp.sum(weights, axis=-1, keepdims=True))
            mixed_blk = jnp.einsum('hqk,khd->qhd', round_trip(weights), values)
            mixed_blk = mixed_blk / jnp.transpose(row_total, (1, 0, 2))
            return (unused, (mixed_blk, (row_max + jnp.log(row_total))[:, :, 0]))
        unused, (mixed_blocks, lse_blocks) = lax.scan(forward_block, jnp.zeros((), jnp.float32), jnp.arange(length // q_rows, dtype=jnp.int32))
        mixed_low = mixed_blocks.reshape(length, D).astype(jnp.bfloat16)
        mixed_back = lax.optimization_barrier(mixed_low).astype(jnp.float32)
        log_total = jnp.transpose(lse_blocks, (1, 0, 2)).reshape(HEADS, length)
        middle = inputs + jnp.dot(mixed_low, w_out, preferred_element_type=jnp.float32) + bias_out

        def mlp_block(totals, block_index):
            offset = block_index * t_rows
            middle_blk = lax.dynamic_slice_in_dim(middle, offset, t_rows, 0)
            grad_blk = lax.dynamic_slice_in_dim(grad_output, offset, t_rows, 0)
            normed_two, pull_two = jax.vjp(layer_norm, middle_blk, gain_two, shift_two)
            normed_two_low = normed_two.astype(jnp.bfloat16)
            pre_act = jnp.dot(normed_two_low, fc_weight, preferred_element_type=jnp.float32) + fc_bias
            activated, pull_gelu = jax.vjp(gelu_tanh, pre_act)
            act_low = activated.astype(jnp.bfloat16)
            output_blk = middle_blk + jnp.dot(act_low, down_weight.T, preferred_element_type=jnp.float32) + bias_proj
            grad_low = grad_blk.astype(jnp.bfloat16)
            d_act = jnp.dot(grad_low, down_weight, preferred_element_type=jnp.float32)
            d_pre = pull_gelu(d_act)[0]
            d_pre_low = d_pre.astype(jnp.bfloat16)
            d_normed_two = jnp.dot(d_pre_low, fc_weight.T, preferred_element_type=jnp.float32)
            d_middle_norm, grad_gain, grad_shift = pull_two(d_normed_two)
            fc_total, down_total, gain_total, shift_total, pre_total, cot_total = totals
            totals = (fc_total + jnp.dot(normed_two_low.T, d_pre_low, preferred_element_type=jnp.float32), down_total + jnp.dot(grad_low.T, act_low, preferred_element_type=jnp.float32), gain_total + grad_gain, shift_total + grad_shift, pre_total + lax.optimization_barrier(jnp.sum(d_pre, axis=0)), cot_total + lax.optimization_barrier(jnp.sum(grad_blk, axis=0)))
            return (totals, (output_blk, grad_blk + d_middle_norm))
        mlp_totals, (output_blocks, d_middle_blocks) = lax.scan(mlp_block, mlp_totals, jnp.arange(length // t_rows, dtype=jnp.int32))
        d_middle = d_middle_blocks.reshape(length, D)
        d_middle_low = d_middle.astype(jnp.bfloat16)
        grad_out_proj = grad_out_proj + jnp.dot(mixed_low.T, d_middle_low, preferred_element_type=jnp.float32)
        d_mixed = round_trip(jnp.dot(d_middle_low, w_out.T, preferred_element_type=jnp.float32)).reshape(length, HEADS, HEAD_DIM)
        mixed_heads = mixed_back.reshape(length, HEADS, HEAD_DIM)
        delta = jnp.einsum('qhd,qhd->hq', d_mixed, mixed_heads)

        def backward_block(carry_in, block_index):
            d_keys, d_values = carry_in
            offset = block_index * q_rows
            query_blk = lax.dynamic_slice_in_dim(queries, offset, q_rows, 0)
            d_mixed_blk = lax.dynamic_slice_in_dim(d_mixed, offset, q_rows, 0)
            lse_blk = lax.dynamic_slice_in_dim(log_total, offset, q_rows, 1)
            delta_blk = lax.dynamic_slice_in_dim(delta, offset, q_rows, 1)
            scores = jnp.einsum('qhd,khd->hqk', query_blk, keys) * score_scale
            allowed = positions[None, :] <= (offset + jnp.arange(q_rows, dtype=jnp.int32))[:, None]
            scores = jnp.where(allowed[None], scores, -jnp.inf)
            probs = jnp.exp(scores - lse_blk[:, :, None])
            probs_low = round_trip(probs)
            d_values = d_values + jnp.einsum('hqk,qhd->khd', probs_low, d_mixed_blk)
            d_probs = jnp.einsum('qhd,khd->hqk', d_mixed_blk, values)
            d_scores = round_trip(probs * (d_probs - delta_blk[:, :, None]) * score_scale)
            d_query_blk = jnp.einsum('hqk,khd->qhd', d_scores, keys)
            d_keys = d_keys + jnp.einsum('hqk,qhd->khd', d_scores, query_blk)
            return ((d_keys, d_values), d_query_blk)
        zero_heads = jnp.zeros((length, HEADS, HEAD_DIM), jnp.float32)
        (d_keys, d_values), d_query_blocks = lax.scan(backward_block, (zero_heads, zero_heads), jnp.arange(length // q_rows, dtype=jnp.int32))
        d_queries = d_query_blocks.reshape(length, D)
        d_keys = d_keys.reshape(length, D)
        d_values = d_values.reshape(length, D)
        d_projected_low = jnp.concatenate([d_queries, d_keys, d_values], axis=1).astype(jnp.bfloat16)
        grad_qkv = grad_qkv + jnp.dot(normed_low.T, d_projected_low, preferred_element_type=jnp.float32)
        d_normed_one = jnp.dot(d_projected_low, w_qkv.T, preferred_element_type=jnp.float32)
        d_input_norm, grad_gain_one, grad_shift_one = pull_one(d_normed_one)
        vec_totals = [vec_totals[0] + grad_gain_one, vec_totals[1] + grad_shift_one, vec_totals[2] + lax.optimization_barrier(jnp.sum(d_queries, axis=0)), vec_totals[3] + lax.optimization_barrier(jnp.sum(d_values, axis=0)), vec_totals[4] + lax.optimization_barrier(jnp.sum(d_middle, axis=0))]
        outputs_list.append(output_blocks.reshape(length, D))
        grads_list.append(d_middle + d_input_norm)
    fc_total, down_total, gain_total, shift_total, pre_total, cot_total = mlp_totals
    vector_grad = jnp.concatenate(vec_totals + [gain_total, shift_total, cot_total, pre_total])
    attn_grad = jnp.concatenate([grad_qkv, grad_out_proj], axis=1)
    return (jnp.stack(outputs_list), jnp.stack(grads_list), attn_grad, fc_total, down_total, vector_grad)
```

```python
import functools
import math

import jax
import jax.numpy as jnp
from jax import lax
from jax.experimental import pallas as pl
from jax.experimental.pallas import tpu as pltpu
from jax.sharding import PartitionSpec as P

D = 1600
HEADS = 25
HEAD_DIM = 64
GROUPS = 13
WIDE = GROUPS * 128

epsilon = 1e-05
gelu_coeff = 0.7978845608028654
MESH = pl.DeviceIdType.MESH
f32, bf16 = jnp.float32, jnp.bfloat16


def place():
    me = lax.axis_index("ctx")
    return me, me // 4, (me // 2) % 2, me % 2


def greet(targets):
    barrier = pltpu.get_barrier_semaphore()
    count = 0
    for ok, t in targets:
        if ok is None:
            pl.semaphore_signal(barrier, inc=1, device_id={"ctx": t}, device_id_type=MESH)
            count = count + 1
        else:
            @pl.when(ok)
            def _(t=t):
                pl.semaphore_signal(barrier, inc=1, device_id={"ctx": t}, device_id_type=MESH)
            count = count + jnp.where(ok, 1, 0)
    pl.semaphore_wait(barrier, count)


def product(acc, a, b_ref):
    width = b_ref.shape[1]
    first = 0
    while first < width:
        last = width if width - first < 1024 else first + 512
        acc[:, first:last] = lax.dot_general(
            a, b_ref[:, first:last], (((1,), (0,)), ((), ())), preferred_element_type=jnp.float32)
        first = last


def rows_of(rows, fn, c, step=16):
    @pl.loop(0, rows // step)
    def _(i):
        fn(pl.ds(pl.multiple_of(c * rows + i * step, step), step))


def gather_kernel(Z, C, x_ref, out_ref, ssem, rsem, lsem):
    me, z, y, k = place()
    rows = x_ref.shape[0] // C
    right, left = jnp.minimum(me + 4, 4 * Z - 1), jnp.maximum(me - 4, 0)
    ypart, cpart = me + 2 - 4 * y, me + 1 - 2 * k
    has_r, has_l = z < Z - 1, z > 0
    greet([(has_r, right), (has_l, left), (None, ypart), (None, cpart)])
    local = pltpu.make_async_copy(x_ref, out_ref.at[me], lsem)
    local.start()
    where = (right, left, ypart, cpart)

    def desc(d, slot, c, src=None):
        part = out_ref.at[slot, pl.ds(c * rows, rows)]
        return pltpu.make_async_remote_copy(
            src_ref=part if src is None else src, dst_ref=part,
            send_sem=ssem.at[d, slot, c], recv_sem=rsem.at[d, slot, c],
            device_id={"ctx": where[d]}, device_id_type=MESH)

    for c in range(C):
        own = x_ref.at[pl.ds(c * rows, rows)]

        @pl.when(has_r)
        def _():
            desc(0, me, c, own).start()

        @pl.when(has_l)
        def _():
            desc(1, me, c, own).start()
        desc(2, me, c, own).start()
        desc(3, me, c, own).start()

    def slot_of(zz, yy, kk):
        return zz * 4 + yy * 2 + kk

    def from_y(zz, c):
        s = slot_of(zz, 1 - y, k)
        desc(2, s, c).wait_recv()
        desc(3, s, c).start()

    def from_y_at(t, c):
        @pl.when(z - t >= 0)
        def _():
            from_y(z - t, c)
        if t > 0:
            @pl.when(z + t <= Z - 1)
            def _():
                from_y(z + t, c)

    for t in range(Z - 1):
        for c in range(C):
            @pl.when(z - 1 - t >= 0)
            def _():
                s = slot_of(z - 1 - t, y, k)
                desc(0, s, c).wait_recv()

                @pl.when(has_r)
                def _():
                    desc(0, s, c).start()
                desc(2, s, c).start()
                desc(3, s, c).start()

            @pl.when(z + 1 + t <= Z - 1)
            def _():
                s = slot_of(z + 1 + t, y, k)
                desc(1, s, c).wait_recv()

                @pl.when(has_l)
                def _():
                    desc(1, s, c).start()
                desc(2, s, c).start()
                desc(3, s, c).start()
            from_y_at(t, c)
    for c in range(C):
        from_y_at(Z - 1, c)
    local.wait()
    for zz in range(Z):
        for c in range(C):
            for yy in range(2):
                desc(3, slot_of(zz, yy, 1 - k), c).wait_recv()
                desc(3, slot_of(zz, yy, k), c).wait_send()
            desc(2, slot_of(zz, y, k), c).wait_send()

            @pl.when((zz <= z) & has_r)
            def _():
                desc(0, slot_of(zz, y, k), c).wait_send()

            @pl.when((zz >= z) & has_l)
            def _():
                desc(1, slot_of(zz, y, k), c).wait_send()


def gather_ctx(x, Z, C, cid):
    n = 4 * Z
    dma = pltpu.SemaphoreType.DMA
    return pl.pallas_call(
        functools.partial(gather_kernel, Z, C),
        out_shape=jax.ShapeDtypeStruct((n,) + x.shape, x.dtype),
        in_specs=[pl.BlockSpec(memory_space=pltpu.VMEM)],
        out_specs=pl.BlockSpec(memory_space=pl.ANY),
        scratch_shapes=[dma((4, n, C)), dma((4, n, C)), dma],
        compiler_params=pltpu.CompilerParams(collective_id=cid, has_side_effects=True),
        name="gather_ctx",
    )(x)


def gather_cube_kernel(x_ref, out_ref, ssem, rsem, lsem):
    me, z, y, k = place()
    zl = z % 2
    rows = x_ref.shape[0] // 2
    zpart, ypart, cpart = me + 4 - 8 * zl, me + 2 - 4 * y, me + 1 - 2 * k
    greet([(None, zpart), (None, ypart), (None, cpart)])
    own = me % 8
    local = pltpu.make_async_copy(x_ref, out_ref.at[own], lsem)
    local.start()
    where = (zpart, ypart, cpart)

    def desc(d, slot, c, src=None):
        part = out_ref.at[slot, pl.ds(c * rows, rows)]
        return pltpu.make_async_remote_copy(
            src_ref=part if src is None else src, dst_ref=part,
            send_sem=ssem.at[d, slot, c], recv_sem=rsem.at[d, slot, c],
            device_id={"ctx": where[d]}, device_id_type=MESH)

    def slot_of(a, b, kk):
        return a * 4 + b * 2 + kk
    z_slot, y_slot, far = slot_of(1 - zl, y, k), slot_of(zl, 1 - y, k), slot_of(1 - zl, 1 - y, k)
    for c in (0, 1):
        half = x_ref.at[pl.ds(c * rows, rows)]
        desc(c, own, c, half).start()
        desc(1 - c, own, c, half).start()
    for c in (0, 1):
        desc(2, own, c, x_ref.at[pl.ds(c * rows, rows)]).start()
    desc(0, z_slot, 0).wait_recv()
    desc(1, z_slot, 0).start()
    desc(1, y_slot, 1).wait_recv()
    desc(0, y_slot, 1).start()
    desc(2, z_slot, 0).start()
    desc(2, y_slot, 1).start()
    desc(0, z_slot, 1).wait_recv()
    desc(2, z_slot, 1).start()
    desc(1, y_slot, 0).wait_recv()
    desc(2, y_slot, 0).start()
    desc(1, far, 0).wait_recv()
    desc(2, far, 0).start()
    desc(0, far, 1).wait_recv()
    desc(2, far, 1).start()
    local.wait()
    for a in range(2):
        for b in range(2):
            for c in range(2):
                desc(2, slot_of(a, b, 1 - k), c).wait_recv()
                desc(2, slot_of(a, b, k), c).wait_send()
    for c in (0, 1):
        desc(0, own, c).wait_send()
        desc(1, own, c).wait_send()
    desc(1, z_slot, 0).wait_send()
    desc(0, y_slot, 1).wait_send()


def gather_cube(x, cid):
    dma = pltpu.SemaphoreType.DMA
    return pl.pallas_call(
        gather_cube_kernel,
        out_shape=jax.ShapeDtypeStruct((8,) + x.shape, x.dtype),
        in_specs=[pl.BlockSpec(memory_space=pltpu.VMEM)],
        out_specs=pl.BlockSpec(memory_space=pl.ANY),
        scratch_shapes=[dma((3, 8, 2)), dma((3, 8, 2)), dma],
        compiler_params=pltpu.CompilerParams(collective_id=cid, has_side_effects=True),
        name="gather_cube",
    )(x)


def scatter_kernel(C, a_ref, b_ref, o_ref, acc, stage, rc, ry, rz, cs, cr, ys, yr, zs, zr):
    me, z, y, k = place()
    Z = 4
    R = a_ref.shape[1]
    rows = R // C
    f = jnp.float32
    right, left = jnp.minimum(me + 4, 4 * Z - 1), jnp.maximum(me - 4, 0)
    ypart, cpart = me + 2 - 4 * y, me + 1 - 2 * k
    has_r, has_l = z < Z - 1, z > 0
    greet([(has_r, right), (has_l, left), (None, ypart), (None, cpart)])

    def target(i):
        end = (z == 0) | (z == Z - 1)
        v = jnp.where(end, 3 - i, jnp.where(i == 0, 3, jnp.where(i == 1, 0, jnp.where(i == 2, 2, 1))))
        return jnp.where(z < 2, v, 3 - v)

    def cd(zz, far, c):
        ds = pl.ds(c * rows, rows)
        s = zz * 2 + far
        return pltpu.make_async_remote_copy(
            src_ref=stage.at[s, ds], dst_ref=rc.at[s, ds], send_sem=cs.at[s, c], recv_sem=cr.at[s, c],
            device_id={"ctx": cpart}, device_id_type=MESH)

    def yd(zz, c):
        ds = pl.ds(c * rows, rows)
        return pltpu.make_async_remote_copy(
            src_ref=rc.at[zz * 2 + 1, ds], dst_ref=ry.at[zz, ds], send_sem=ys.at[zz, c], recv_sem=yr.at[zz, c],
            device_id={"ctx": ypart}, device_id_type=MESH)

    def zd(d, zz, c, first=False):
        ds = pl.ds(c * rows, rows)
        return pltpu.make_async_remote_copy(
            src_ref=ry.at[zz, ds] if first else rz.at[d, zz, ds], dst_ref=rz.at[d, zz, ds],
            send_sem=zs.at[d, zz, c], recv_sem=zr.at[d, zz, c],
            device_id={"ctx": (right, left)[d]}, device_id_type=MESH)

    def slot(zz, far, kk):
        return zz * 4 + (y + far - 2 * y * far) * 2 + kk

    for far in (1, 0):
        @pl.loop(0, Z)
        def _(i):
            zz = target(i)
            product(acc, a_ref[slot(zz, far, 1 - k)], b_ref)
            for c in range(C):
                def move(ds):
                    stage[zz * 2 + far, ds, :] = acc[ds, :].astype(stage.dtype)
                rows_of(rows, move, c)
                cd(zz, far, c).start()
        if far:
            continue

    @pl.loop(0, Z)
    def _(i):
        zz = target(i)
        product(acc, a_ref[slot(zz, 1, k)], b_ref)
        for c in range(C):
            cd(zz, 1, c).wait_recv()

            def join(ds):
                s = zz * 2 + 1
                rc[s, ds, :] = (rc[s, ds, :].astype(f) + acc[ds, :]).astype(rc.dtype)
            rows_of(rows, join, c)
            yd(zz, c).start()

    @pl.loop(0, Z - 1)
    def _(i):
        zz = target(i)
        product(acc, a_ref[slot(zz, 0, k)], b_ref)
        for c in range(C):
            cd(zz, 0, c).wait_recv()
            yd(zz, c).wait_recv()

            def join(ds):
                ry[zz, ds, :] = (acc[ds, :] + rc[zz * 2, ds, :].astype(f) + ry[zz, ds, :].astype(f)).astype(ry.dtype)
            rows_of(rows, join, c)
            for d, here, starts in ((0, zz > z, z == 0), (1, zz < z, z == Z - 1)):
                @pl.when(here & starts)
                def _():
                    zd(d, zz, c, True).start()

                @pl.when(here & jnp.logical_not(starts))
                def _():
                    zd(d, zz, c).wait_recv()

                    def add(ds):
                        rz[d, zz, ds, :] = (rz[d, zz, ds, :].astype(f) + ry[zz, ds, :].astype(f)).astype(rz.dtype)
                    rows_of(rows, add, c)
                    zd(d, zz, c).start()

    product(acc, a_ref[slot(z, 0, k)], b_ref)
    for c in range(C):
        cd(z, 0, c).wait_recv()
        yd(z, c).wait_recv()

        def join(ds):
            o_ref[ds, :] = acc[ds, :] + rc[z * 2, ds, :].astype(f) + ry[z, ds, :].astype(f)
        rows_of(rows, join, c)
        for d, here in ((0, has_l), (1, has_r)):
            @pl.when(here)
            def _():
                zd(d, z, c).wait_recv()

                def add(ds):
                    o_ref[ds, :] += rz[d, z, ds, :].astype(f)
                rows_of(rows, add, c)
    for c in range(C):
        @pl.loop(0, Z)
        def _(zz):
            for far in (0, 1):
                cd(zz, far, c).wait_send()
            yd(zz, c).wait_send()

            @pl.when(zz > z)
            def _():
                zd(0, zz, c).wait_send()

            @pl.when(zz < z)
            def _():
                zd(1, zz, c).wait_send()


def scatter_ctx(a, b, C, cid):
    n, R, _ = a.shape
    N, Z = b.shape[1], 4
    dma = pltpu.SemaphoreType.DMA
    vm = pl.BlockSpec(memory_space=pltpu.VMEM)
    low = jnp.bfloat16
    return pl.pallas_call(
        functools.partial(scatter_kernel, C),
        out_shape=jax.ShapeDtypeStruct((R, N), jnp.float32),
        in_specs=[vm, vm],
        out_specs=vm,
        scratch_shapes=[
            pltpu.VMEM((R, N), jnp.float32), pltpu.VMEM((2 * Z, R, N), low), pltpu.VMEM((2 * Z, R, N), low), pltpu.VMEM((Z, R, N), low),
            pltpu.VMEM((2, Z, R, N), low), dma((2 * Z, C)), dma((2 * Z, C)), dma((Z, C)), dma((Z, C)), dma((2, Z, C)), dma((2, Z, C)),
        ],
        compiler_params=pltpu.CompilerParams(collective_id=cid, has_side_effects=True, vmem_limit_bytes=60 << 20),
        name="scatter_ctx",
    )(a, b)


def scatter_cube_kernel(a_ref, b_ref, o_ref, acc, stage, rc, rz, ry, cs, cr, zs, zr, ys, yr):
    me, z, y, k = place()
    zl = z % 2
    R = a_ref.shape[1]
    rows = R // 2
    f = jnp.float32
    zpart, ypart, cpart = me + 4 - 8 * zl, me + 2 - 4 * y, me + 1 - 2 * k
    greet([(None, zpart), (None, ypart), (None, cpart)])
    FAR, ZN, YN, OWN = range(4)

    def slot(i, kk):
        flip_z = jnp.where(i < 2, 1, 0)
        flip_y = jnp.where((i == 0) | (i == 2), 1, 0)
        return (zl + flip_z - 2 * zl * flip_z) * 4 + (y + flip_y - 2 * y * flip_y) * 2 + kk

    def cd(i):
        return pltpu.make_async_remote_copy(
            src_ref=stage.at[i], dst_ref=rc.at[i], send_sem=cs.at[i], recv_sem=cr.at[i],
            device_id={"ctx": cpart}, device_id_type=MESH)

    def link(over_z, i, c, dst):
        land, ss, rs = (rz, zs, zr) if over_z else (ry, ys, yr)
        return pltpu.make_async_remote_copy(
            src_ref=rc.at[i, pl.ds(c * rows, rows)], dst_ref=land.at[dst], send_sem=ss.at[dst], recv_sem=rs.at[dst],
            device_id={"ctx": zpart if over_z else ypart}, device_id_type=MESH)

    @pl.loop(0, 4)
    def _(i):
        product(acc, a_ref[slot(i, 1 - k)], b_ref)

        def move(ds):
            stage[i, ds, :] = acc[ds, :].astype(stage.dtype)
        rows_of(R, move, 0)
        cd(i).start()

    def chip_sum(i):
        product(acc, a_ref[slot(i, k)], b_ref)
        cd(i).wait_recv()

        def join(ds):
            rc[i, ds, :] = (rc[i, ds, :].astype(f) + acc[ds, :]).astype(rc.dtype)
        rows_of(R, join, 0)

    def pass_on(land, i, c):
        def add(ds):
            dst = pl.ds(pl.multiple_of(ds.start - c * rows, 16), 16)
            rc[i, ds, :] = (rc[i, ds, :].astype(f) + land[2, dst, :].astype(f)).astype(rc.dtype)
        rows_of(rows, add, c)

    chip_sum(FAR)
    link(True, FAR, 0, 2).start()
    link(False, FAR, 1, 2).start()
    chip_sum(ZN)
    link(True, ZN, 0, 0).start()
    chip_sum(YN)
    link(False, YN, 1, 1).start()
    link(True, FAR, 0, 2).wait_recv()
    pass_on(rz, YN, 0)
    link(False, YN, 0, 0).start()
    link(False, FAR, 1, 2).wait_recv()
    pass_on(ry, ZN, 1)
    link(True, ZN, 1, 1).start()
    product(acc, a_ref[slot(OWN, k)], b_ref)
    cd(OWN).wait_recv()

    def join(ds):
        o_ref[ds, :] = acc[ds, :] + rc[OWN, ds, :].astype(f)
    rows_of(R, join, 0)
    for over_z, c in ((True, 0), (False, 1), (False, 0), (True, 1)):
        link(over_z, OWN, c, c).wait_recv()
        land = rz if over_z else ry

        def add(ds):
            dst = pl.ds(pl.multiple_of(ds.start - c * rows, 16), 16)
            o_ref[ds, :] += land[c, dst, :].astype(f)
        rows_of(rows, add, c)
    for i in range(4):
        cd(i).wait_send()
    for over_z in (True, False):
        for dst in range(3):
            link(over_z, FAR, 0, dst).wait_send()


def scatter_cube(a, b, cid):
    n, R, _ = a.shape
    N = b.shape[1]
    dma = pltpu.SemaphoreType.DMA
    vm = pl.BlockSpec(memory_space=pltpu.VMEM)
    low = jnp.bfloat16
    return pl.pallas_call(
        scatter_cube_kernel,
        out_shape=jax.ShapeDtypeStruct((R, N), jnp.float32),
        in_specs=[vm, vm],
        out_specs=vm,
        scratch_shapes=[
            pltpu.VMEM((R, N), jnp.float32), pltpu.VMEM((4, R, N), low), pltpu.VMEM((4, R, N), low), pltpu.VMEM((3, R // 2, N), low),
            pltpu.VMEM((3, R // 2, N), low), dma((4,)), dma((4,)), dma((3,)), dma((3,)), dma((3,)), dma((3,)),
        ],
        compiler_params=pltpu.CompilerParams(collective_id=cid, has_side_effects=True, vmem_limit_bytes=60 << 20),
        name="scatter_cube",
    )(a, b)


def greet_all(n_x, n_c):
    barrier = pltpu.get_barrier_semaphore()
    me = lax.axis_index("fsdp") * n_c + lax.axis_index("ctx")
    n = n_x * n_c

    @pl.loop(1, n)
    def _(i):
        d = (me + i) % n
        pl.semaphore_signal(barrier, inc=1, device_id={"fsdp": d // n_c, "ctx": d % n_c}, device_id_type=MESH)
    pl.semaphore_wait(barrier, n - 1)


def spread_kernel(n_x, n_c, wt_ref, vec_ref, wh_ref, wout_ref, vall_ref, us, ur, os, orr, vs, vr, ls):
    x, ctx = lax.axis_index("fsdp"), lax.axis_index("ctx")
    n = n_x * n_c
    me = x * n_c + ctx
    U = wt_ref.shape[0]
    first_out = 3 * n // 4
    per = U * n // 4
    greet_all(n_x, n_c)

    def vec_copy(i, sending):
        d = (me + i) % n if sending else (me + n - i) % n
        slot = me if sending else d
        return pltpu.make_async_remote_copy(
            src_ref=vec_ref, dst_ref=vall_ref.at[slot], send_sem=vs.at[i], recv_sem=vr.at[slot],
            device_id={"fsdp": d // n_c, "ctx": d % n_c}, device_id_type=MESH)

    @pl.loop(1, n)
    def _(i):
        vec_copy(i, True).start()
    own_vec = pltpu.make_async_copy(vec_ref, vall_ref.at[me], ls)
    own_vec.start()

    def unit_target(u):
        g = U * me + u
        return (g % per) // 16, (g // per) * 16 + (g % per) % 16

    def unit_copy(u, to_x, j, slot):
        return pltpu.make_async_remote_copy(
            src_ref=wt_ref.at[u], dst_ref=wh_ref.at[slot], send_sem=us.at[u, to_x], recv_sem=ur.at[slot],
            device_id={"fsdp": to_x, "ctx": j}, device_id_type=MESH)

    def unit_local(u, slot):
        return pltpu.make_async_copy(wt_ref.at[u], wh_ref.at[slot], ur.at[slot])

    def out_copy(j, to_x, o):
        return pltpu.make_async_remote_copy(
            src_ref=wt_ref.at[:, :, pl.ds(pl.multiple_of(j * 128, 128), 128)], dst_ref=wout_ref.at[pl.ds(U * o, U)],
            send_sem=os.at[j, to_x], recv_sem=orr.at[o], device_id={"fsdp": to_x, "ctx": j}, device_id_type=MESH)

    def out_local(j, o):
        return pltpu.make_async_copy(
            wt_ref.at[:, :, pl.ds(pl.multiple_of(j * 128, 128), 128)], wout_ref.at[pl.ds(U * o, U)], orr.at[o])

    def sends(remote, local):
        @pl.when(me < first_out)
        def _():
            @pl.loop(0, U)
            def _(u):
                j, slot = unit_target(u)
                for to_x in range(n_x):
                    here = (x == to_x) & (ctx == j)

                    @pl.when(jnp.logical_not(here))
                    def _():
                        remote(unit_copy(u, to_x, j, slot))
                    if local is not None:
                        @pl.when(here)
                        def _():
                            local(unit_local(u, slot))

        @pl.when(me >= first_out)
        def _():
            @pl.loop(0, GROUPS)
            def _(j):
                for to_x in range(n_x):
                    here = (x == to_x) & (ctx == j)

                    @pl.when(jnp.logical_not(here))
                    def _():
                        remote(out_copy(j, to_x, me - first_out))
                    if local is not None:
                        @pl.when(here)
                        def _():
                            local(out_local(j, me - first_out))

    sends(lambda c: c.start(), lambda c: c.start())
    own_vec.wait()

    @pl.loop(1, n)
    def _(i):
        vec_copy(i, False).wait_recv()

    @pl.when(ctx < GROUPS)
    def _():
        @pl.loop(0, 48)
        def _(slot):
            e = ctx * 16 + slot % 16
            g = (slot // 16) * per + e
            owner = g // U

            @pl.when(e < per)
            def _():
                @pl.when(owner == me)
                def _():
                    unit_local(g % U, slot).wait()

                @pl.when(owner != me)
                def _():
                    unit_copy(g % U, 1 - x, ctx, slot).wait_recv()

        @pl.loop(0, n // 4)
        def _(o):
            @pl.when(o + first_out == me)
            def _():
                out_local(ctx, o).wait()

            @pl.when(o + first_out != me)
            def _():
                out_copy(ctx, 1 - x, o).wait_recv()

    @pl.loop(1, n)
    def _(i):
        vec_copy(i, True).wait_send()
    sends(lambda c: c.wait_send(), None)


def spread(wt, vec, n_x, n_c, cid):
    n = n_x * n_c
    U = wt.shape[0]
    dma = pltpu.SemaphoreType.DMA
    vm, hbm = pl.BlockSpec(memory_space=pltpu.VMEM), pl.BlockSpec(memory_space=pl.ANY)
    return pl.pallas_call(
        functools.partial(spread_kernel, n_x, n_c),
        out_shape=(
            jax.ShapeDtypeStruct((48, 8, WIDE), bf16),
            jax.ShapeDtypeStruct((U * n // 4, 8, 128), bf16),
            jax.ShapeDtypeStruct((n, 8, 128), f32),
        ),
        in_specs=[vm, vm],
        out_specs=(hbm, hbm, hbm),
        scratch_shapes=[dma((U, n_x)), dma((48,)), dma((GROUPS, n_x)), dma((n // 4,)), dma((n,)), dma((n,)), dma],
        compiler_params=pltpu.CompilerParams(collective_id=cid, has_side_effects=True),
        name="spread",
    )(wt, vec)


def collect_kernel(n_x, n_c, U, gh_ref, gout_ref, r_ref, us, ur, os, orr):
    x, ctx = lax.axis_index("fsdp"), lax.axis_index("ctx")
    n = n_x * n_c
    me = x * n_c + ctx
    first_out = 3 * n // 4
    per = U * n // 4
    greet_all(n_x, n_c)

    def unit_copy(from_x, slot, owner, u):
        return pltpu.make_async_remote_copy(
            src_ref=gh_ref.at[slot], dst_ref=r_ref.at[from_x, u], send_sem=us.at[slot], recv_sem=ur.at[from_x, u],
            device_id={"fsdp": owner // n_c, "ctx": owner % n_c}, device_id_type=MESH)

    def unit_local(slot, u):
        return pltpu.make_async_copy(gh_ref.at[slot], r_ref.at[x, u], ur.at[x, u])

    def out_copy(from_x, j, o):
        owner = first_out + o
        return pltpu.make_async_remote_copy(
            src_ref=gout_ref.at[pl.ds(U * o, U)], dst_ref=r_ref.at[from_x, :, :, pl.ds(pl.multiple_of(j * 128, 128), 128)],
            send_sem=os.at[o], recv_sem=orr.at[from_x, j],
            device_id={"fsdp": owner // n_c, "ctx": owner % n_c}, device_id_type=MESH)

    def out_local(j, o):
        return pltpu.make_async_copy(
            gout_ref.at[pl.ds(U * o, U)], r_ref.at[x, :, :, pl.ds(pl.multiple_of(j * 128, 128), 128)], orr.at[x, j])

    def sends(remote, local):
        @pl.when(ctx < GROUPS)
        def _():
            @pl.loop(0, 48)
            def _(slot):
                e = ctx * 16 + slot % 16
                g = (slot // 16) * per + e

                @pl.when((e < per) & (g // U != me))
                def _():
                    remote(unit_copy(x, slot, g // U, g % U))
                if local is not None:
                    @pl.when((e < per) & (g // U == me))
                    def _():
                        local(unit_local(slot, g % U))

            @pl.loop(0, n // 4)
            def _(o):
                @pl.when(o + first_out != me)
                def _():
                    remote(out_copy(x, ctx, o))
                if local is not None:
                    @pl.when(o + first_out == me)
                    def _():
                        local(out_local(ctx, o))

    sends(lambda c: c.start(), lambda c: c.start())

    @pl.when(me < first_out)
    def _():
        for from_x in range(n_x):
            @pl.loop(0, U)
            def _(u):
                g = U * me + u
                j, slot = (g % per) // 16, (g // per) * 16 + (g % per) % 16
                here = (x == from_x) & (ctx == j)

                @pl.when(here)
                def _():
                    unit_local(slot, u).wait()

                @pl.when(jnp.logical_not(here))
                def _():
                    unit_copy(from_x, slot, (me + 1) % n, u).wait_recv()

    @pl.when(me >= first_out)
    def _():
        for from_x in range(n_x):
            @pl.loop(0, GROUPS)
            def _(j):
                here = (x == from_x) & (ctx == j)

                @pl.when(here)
                def _():
                    out_local(j, me - first_out).wait()

                @pl.when(jnp.logical_not(here))
                def _():
                    out_copy(from_x, j, 0).wait_recv()
    sends(lambda c: c.wait_send(), None)


def collect(gh, gout, n_x, n_c, cid):
    n = n_x * n_c
    U = gout.shape[0] * 4 // n
    dma = pltpu.SemaphoreType.DMA
    hbm = pl.BlockSpec(memory_space=pl.ANY)
    return pl.pallas_call(
        functools.partial(collect_kernel, n_x, n_c, U),
        out_shape=jax.ShapeDtypeStruct((n_x, U, 8, WIDE), bf16),
        in_specs=[hbm, hbm],
        out_specs=hbm,
        scratch_shapes=[dma((48,)), dma((n_x, U)), dma((n // 4,)), dma((n_x, GROUPS))],
        compiler_params=pltpu.CompilerParams(collective_id=cid, has_side_effects=True),
        name="collect",
    )(gh, gout)


def reduce_kernel(n_x, n_c, p_ref, o_ref, land, ss, rs):
    n = n_x * n_c
    me = lax.axis_index("fsdp") * n_c + lax.axis_index("ctx")
    greet_all(n_x, n_c)

    def copy(i, sending):
        d = (me + i) % n if sending else (me + n - i) % n
        return pltpu.make_async_remote_copy(
            src_ref=p_ref.at[d], dst_ref=land.at[i], send_sem=ss.at[i], recv_sem=rs.at[i],
            device_id={"fsdp": d // n_c, "ctx": d % n_c}, device_id_type=MESH)

    @pl.loop(1, n)
    def _(i):
        copy(i, True).start()

    @pl.loop(1, n)
    def _(i):
        copy(i, False).wait_recv()
    o_ref[...] = lax.fori_loop(1, n, lambda i, s: s + land[i], p_ref[me])

    @pl.loop(1, n)
    def _(i):
        copy(i, True).wait_send()


def reduce_vectors(p, n_x, n_c, cid):
    n = n_x * n_c
    dma = pltpu.SemaphoreType.DMA
    vm = pl.BlockSpec(memory_space=pltpu.VMEM)
    return pl.pallas_call(
        functools.partial(reduce_kernel, n_x, n_c),
        out_shape=jax.ShapeDtypeStruct(p.shape[1:], f32),
        in_specs=[vm],
        out_specs=vm,
        scratch_shapes=[pltpu.VMEM(p.shape, f32), dma((n,)), dma((n,))],
        compiler_params=pltpu.CompilerParams(collective_id=cid, has_side_effects=True),
        name="reduce_vectors",
    )(p)


def dot(a, b, dims):
    return lax.dot_general(a, b, (dims, ((), ())), preferred_element_type=f32)

def attn_fwd_kernel(B, scale, q_ref, k_ref, v_ref, o_ref, lse_ref, qm, vt):
    S = q_ref.shape[0]
    lane = lax.broadcasted_iota(jnp.int32, (1, 128), 1)
    sub = lax.broadcasted_iota(jnp.int32, (128, 1), 0)
    nb = S // B

    @pl.loop(0, nb)
    def _(i):
        ds = pl.ds(pl.multiple_of(i * B, B), B)
        q = q_ref[ds, :].astype(f32) * scale
        v = v_ref[ds, :].astype(f32).T
        for h in range(2):
            qm[h, ds, :] = jnp.where(lane // 64 == h, q, 0.0).astype(bf16)
            vt[h, :, ds] = jnp.where(sub // 64 == h, v, 0.0).astype(bf16)

    row = lax.broadcasted_iota(jnp.int32, (B, B), 0)
    col = lax.broadcasted_iota(jnp.int32, (B, B), 1)

    @pl.loop(0, nb)
    def _(i):
        qs = pl.ds(pl.multiple_of(i * B, B), B)

        def block(j, carry, diag):
            m, l, acc = carry
            ks = pl.ds(pl.multiple_of(j * B, B), B)
            k = k_ref[ks, :]
            new_m, new_l, facs, parts = [], [], [], []
            for h in range(2):
                s = dot(k, qm[h, qs, :], ((1,), (1,)))
                if diag:
                    s = jnp.where(row <= col, s, -jnp.inf)
                mh = jnp.maximum(m[h], jnp.max(s, axis=0, keepdims=True))
                p = jnp.exp(s - mh)
                fac = jnp.exp(m[h] - mh)
                new_m.append(mh)
                new_l.append(l[h] * fac + jnp.sum(p, axis=0, keepdims=True))
                facs.append(fac)
                parts.append(dot(vt[h, :, ks], p.astype(bf16), ((1,), (0,))))
            acc = acc * jnp.where(sub // 64 == 0, facs[0], facs[1]) + (parts[0] + parts[1])
            return tuple(new_m), tuple(new_l), acc

        init = (
            (jnp.full((1, B), -1e30, f32),) * 2,
            (jnp.zeros((1, B), f32),) * 2,
            jnp.zeros((128, B), f32),
        )
        carry = lax.fori_loop(0, i, lambda j, c: block(j, c, False), init)
        m, l, acc = block(i, carry, True)
        acc = acc / jnp.where(sub // 64 == 0, l[0], l[1])
        o_ref[qs, :] = acc.T.astype(bf16)
        for h in range(2):
            lse_ref[pl.ds(h, 1), qs] = m[h] + jnp.log(l[h])

def attn_fwd(q, k, v, B=512, scale=0.125):
    S = q.shape[0]
    return pl.pallas_call(
        functools.partial(attn_fwd_kernel, B, scale),
        out_shape=(jax.ShapeDtypeStruct((S, 128), bf16), jax.ShapeDtypeStruct((2, S), f32)),
        in_specs=[pl.BlockSpec(memory_space=pltpu.VMEM)] * 3,
        out_specs=(pl.BlockSpec(memory_space=pltpu.VMEM),) * 2,
        scratch_shapes=[pltpu.VMEM((2, S, 128), bf16), pltpu.VMEM((2, 128, S), bf16)],
        compiler_params=pltpu.CompilerParams(vmem_limit_bytes=48 << 20),
        cost_estimate=pl.CostEstimate(flops=4 * S * S * 128, bytes_accessed=S * 1024, transcendentals=S * S),
        name="attn_fwd",
    )(q, k, v)

def attn_bwd_kernel(B, scale, q_ref, k_ref, v_ref, g_ref, o_ref, lse_ref, dq_ref, dk_ref, dv_ref, sums_ref, qm, gm, kt, delta, dqt):
    S = q_ref.shape[0]
    lane = lax.broadcasted_iota(jnp.int32, (1, 128), 1)
    sub = lax.broadcasted_iota(jnp.int32, (128, 1), 0)
    nb = S // B

    @pl.loop(0, nb)
    def _(i):
        ds = pl.ds(pl.multiple_of(i * B, B), B)
        q = q_ref[ds, :].astype(f32) * scale
        g = g_ref[ds, :].astype(f32)
        kk = (k_ref[ds, :].astype(f32) * scale).T
        go = (g * o_ref[ds, :].astype(f32)).T
        for h in range(2):
            qm[h, ds, :] = jnp.where(lane // 64 == h, q, 0.0).astype(bf16)
            gm[h, ds, :] = jnp.where(lane // 64 == h, g, 0.0).astype(bf16)
            kt[h, :, ds] = jnp.where(sub // 64 == h, kk, 0.0).astype(bf16)
            delta[pl.ds(h, 1), ds] = jnp.sum(jnp.where(sub // 64 == h, go, 0.0), axis=0, keepdims=True)
        dqt[:, ds] = jnp.zeros((128, B), f32)

    row = lax.broadcasted_iota(jnp.int32, (B, B), 0)
    col = lax.broadcasted_iota(jnp.int32, (B, B), 1)

    def over_keys(j, sum_v):
        ks = pl.ds(pl.multiple_of(j * B, B), B)
        k, v = k_ref[ks, :], v_ref[ks, :]

        def block(i, carry, diag):
            dk, dv = carry
            qs = pl.ds(pl.multiple_of(i * B, B), B)
            upd = None
            for h in range(2):
                q, g = qm[h, qs, :], gm[h, qs, :]
                s = dot(k, q, ((1,), (1,)))
                if diag:
                    s = jnp.where(row <= col, s, -jnp.inf)
                p = jnp.exp(s - lse_ref[pl.ds(h, 1), qs])
                dp = dot(v, g, ((1,), (1,)))
                ds_ = (p * (dp - delta[pl.ds(h, 1), qs])).astype(bf16)
                dv = dv + dot(p.astype(bf16), g, ((1,), (0,)))
                dk = dk + dot(ds_, q, ((1,), (0,)))
                t = dot(kt[h, :, ks], ds_, ((1,), (0,)))
                upd = t if upd is None else upd + t
            dqt[:, qs] += upd
            return dk, dv

        zero = jnp.zeros((B, 128), f32)
        carry = block(j, (zero, zero), True)
        dk, dv = lax.fori_loop(j + 1, nb, lambda i, c: block(i, c, False), carry)
        dk_ref[ks, :] = dk.astype(bf16)
        dv_ref[ks, :] = dv.astype(bf16)
        return sum_v + jnp.sum(dv, axis=0, keepdims=True)

    sum_v = lax.fori_loop(0, nb, over_keys, jnp.zeros((1, 128), f32))

    def finish(i, sum_q):
        ds = pl.ds(pl.multiple_of(i * B, B), B)
        dq = dqt[:, ds].T
        dq_ref[ds, :] = dq.astype(bf16)
        return sum_q + jnp.sum(dq, axis=0, keepdims=True)

    sum_q = lax.fori_loop(0, nb, finish, jnp.zeros((1, 128), f32))
    sums_ref[pl.ds(0, 1), :] = sum_q
    sums_ref[pl.ds(1, 1), :] = sum_v

def attn_bwd(q, k, v, g, o, lse, B=512, scale=0.125):
    S = q.shape[0]
    vm = pl.BlockSpec(memory_space=pltpu.VMEM)
    return pl.pallas_call(
        functools.partial(attn_bwd_kernel, B, scale),
        out_shape=(jax.ShapeDtypeStruct((S, 128), bf16),) * 3 + (jax.ShapeDtypeStruct((2, 128), f32),),
        in_specs=[vm] * 6,
        out_specs=(vm,) * 4,
        scratch_shapes=[pltpu.VMEM((2, S, 128), bf16), pltpu.VMEM((2, S, 128), bf16), pltpu.VMEM((2, 128, S), bf16), pltpu.VMEM((2, S), f32), pltpu.VMEM((128, S), f32)],
        compiler_params=pltpu.CompilerParams(vmem_limit_bytes=56 << 20),
        cost_estimate=pl.CostEstimate(flops=10 * S * S * 128, bytes_accessed=S * 2560, transcendentals=S * S),
        name="attn_bwd",
    )(q, k, v, g, o, lse)


def layer_norm(values, gain_vec, shift_vec):
    center = values - jnp.mean(values, axis=-1, keepdims=True)
    spread_of = jnp.mean(center * center, axis=-1, keepdims=True)
    return center * lax.rsqrt(spread_of + epsilon) * gain_vec + shift_vec


def gelu_tanh(values):
    return 0.5 * values * (1.0 + jnp.tanh(gelu_coeff * (values + 0.044715 * values * values * values)))


def per_device(block_input, attn_weight, fc_weight, down_weight, vectors, cotangent):
    n_x, n_c = lax.axis_size("fsdp"), lax.axis_size("ctx")
    n = n_x * n_c
    x, ctx = lax.axis_index("fsdp"), lax.axis_index("ctx")
    me = x * n_c + ctx
    both = ("fsdp", "ctx")
    inputs, grad_output = block_input[0], cotangent[0]
    rows = inputs.shape[0]
    tokens = rows * n_c
    cols = attn_weight.shape[1]
    owned = vectors.shape[0]
    fast = n_x == 2 and n_c == 16 and cols % 8 == 0 and rows == 128
    ids = iter(range(1, 100))
    half = ctx // 8
    other_x = [(i, (i + 1) % n_x) for i in range(n_x)]
    other_half = [(i, (i + 8) % n_c) for i in range(n_c)]

    def swap_x(part):
        return lax.ppermute(part, "fsdp", other_x)

    def swap_half(part):
        return lax.ppermute(part, "ctx", other_half)

    attn_rows = attn_weight.T
    if fast:
        own_rows = jnp.concatenate([fc_weight.T, down_weight.T])
        half_rows = swap_half(own_rows)
        x_rows = swap_x(own_rows)
        both_rows = swap_x(half_rows)
        four = (own_rows, half_rows, x_rows, both_rows)
        fc_rows = jnp.concatenate([part[:cols] for part in four])
        down_rows = jnp.concatenate([part[cols:] for part in four])
        owners = [me, x * n_c + (ctx + 8) % n_c, (1 - x) * n_c + ctx, (1 - x) * n_c + (ctx + 8) % n_c]
    else:
        fc_rows = lax.all_gather(fc_weight.T, "fsdp", axis=0, tiled=True)
        down_rows = lax.all_gather(down_weight.T, "fsdp", axis=0, tiled=True)
        owners = [i * n_c + ctx for i in range(n_x)]

    def gather(part):
        if fast:
            return gather_ctx(part, n_c // 4, 2, next(ids)).reshape(tokens, -1)
        return lax.all_gather(part, "ctx", axis=0, tiled=True)

    def gather_near(part):
        if fast:
            return gather_cube(part, next(ids)).reshape(8 * rows, -1)
        return lax.all_gather(part, "ctx", axis=0, tiled=True)

    def scatter(left, right):
        if fast:
            return scatter_ctx(left.reshape(n_c, rows, -1), right, 2, next(ids))
        return lax.psum_scatter(dot(left, right, ((1,), (0,))), "ctx", scatter_dimension=0, tiled=True)

    def scatter_near(left, right):
        if fast:
            return scatter_cube(left.reshape(8, rows, -1), right, next(ids))
        return lax.psum_scatter(dot(left, right, ((1,), (0,))), "ctx", scatter_dimension=0, tiled=True)

    if fast:
        wt = jnp.pad(attn_rows, ((0, 0), (0, WIDE - D))).reshape(cols // 8, 8, WIDE)
        vec = jnp.pad(vectors.astype(f32), (0, 1024 - owned)).reshape(8, 128)
        head_units, out_units, vec_all = spread(wt, vec, n_x, n_c, next(ids))
        vec_full = vec_all.reshape(n, 1024)[:, :owned].reshape(-1)
        head_rows = head_units.reshape(3, 128, WIDE)[:, :, :D]
        live = ctx * 128 + jnp.arange(128, dtype=jnp.int32) < D
        head_rows = jnp.where(live[None, :, None], head_rows, 0).reshape(384, D)
        out_rows = jnp.where(live[None, :], out_units.reshape(D, 128), 0)
    else:
        full = lax.all_gather(attn_rows, both, axis=0, tiled=True)
        vec_full = lax.all_gather(vectors, both, axis=0, tiled=True).astype(f32)
        extra = n_c * 128 - D
        head_rows = jnp.pad(full[: 3 * D].reshape(3, D, D), ((0, 0), (0, extra), (0, 0)))
        head_rows = lax.dynamic_slice_in_dim(head_rows, ctx * 128, 128, 1).reshape(384, D)
        out_rows = lax.dynamic_slice_in_dim(jnp.pad(full[3 * D :], ((0, 0), (0, extra))), ctx * 128, 128, 1)

    def vec_at(block):
        return vec_full[block * D : (block + 1) * D]

    def heads_of(block):
        return lax.dynamic_slice_in_dim(jnp.pad(vec_at(block), (0, n_c * 128 - D)), ctx * 128, 128, 0)

    gain_one, shift_one, bias_out = vec_at(0), vec_at(1), vec_at(4)
    gain_two, shift_two, bias_down = vec_at(5), vec_at(6), vec_at(7)
    bias_heads = jnp.concatenate([heads_of(2), jnp.zeros((128,), f32), heads_of(3)])
    up_first = [8 * D + cols * owner for owner in owners]
    bias_up = jnp.concatenate([lax.dynamic_slice_in_dim(vec_full, first, cols, 0) for first in up_first])
    if fast:
        out_rows = jnp.concatenate([out_rows, swap_half(out_rows)], axis=1)
    out_back = out_rows.T

    normed_one, pull_one = jax.vjp(layer_norm, inputs, gain_one, shift_one)
    normed_one_all = gather(normed_one.astype(bf16))
    grad_low = grad_output.astype(bf16)
    normed_one_all, grad_low = lax.optimization_barrier((normed_one_all, grad_low))
    groups = [list(range(8)), list(range(8, 16))] if fast else None
    grad_low_all = lax.all_gather(grad_low, "ctx", axis=0, tiled=True, axis_index_groups=groups)
    qkv = (dot(normed_one_all, head_rows, ((1,), (1,))) + bias_heads).astype(bf16)
    queries, keys, values = qkv[:, :128], qkv[:, 128:256], qkv[:, 256:]
    mixed, log_total = attn_fwd(queries, keys, values, min(1024, tokens))
    mixed_near = mixed
    if fast:
        mixed_halves = mixed.reshape(2, tokens // 2, 128)
        got = swap_half(lax.dynamic_index_in_dim(mixed_halves, 1 - half, 0, False))
        mixed_near = jnp.concatenate([lax.dynamic_index_in_dim(mixed_halves, half, 0, False), got], axis=1)
    middle = inputs + scatter_near(mixed_near, out_back) + bias_out

    normed_two, pull_two = jax.vjp(layer_norm, middle, gain_two, shift_two)
    normed_two_all = gather_near(normed_two.astype(bf16))
    pre_act = dot(normed_two_all, fc_rows, ((1,), (1,))) + bias_up
    activated, pull_gelu = jax.vjp(gelu_tanh, pre_act)
    act_low = activated.astype(bf16)
    d_act = dot(grad_low_all, down_rows, ((1,), (1,)))
    d_pre = pull_gelu(d_act)[0]
    d_pre_low = d_pre.astype(bf16)
    d_normed_two = scatter_near(d_pre_low, fc_rows)
    d_normed_two, act_later = lax.optimization_barrier((d_normed_two, act_low))

    def weight_shard(left, right):
        part = dot(left, right, ((0,), (0,)))
        if fast:
            part = part[: 2 * cols] + swap_x(part[2 * cols :].astype(bf16)).astype(f32)
            return (part[:cols] + swap_half(part[cols:].astype(bf16)).astype(f32)).T
        return lax.psum_scatter(part, "fsdp", scatter_dimension=0, tiled=True).T

    down_shard = weight_shard(act_low, grad_low_all)
    fc_shard = weight_shard(d_pre_low, normed_two_all)

    d_middle_norm, grad_gain_two, grad_shift_two = pull_two(d_normed_two)
    d_middle = grad_output + d_middle_norm
    d_middle_all = gather_near(d_middle.astype(bf16))
    d_mixed = dot(d_middle_all, out_rows, ((1,), (0,))).astype(bf16)
    out_grads = dot(d_middle_all, mixed_near, ((0,), (0,)))
    if fast:
        got = swap_half(d_mixed[:, 128:])
        d_mixed = d_mixed[:, :128]
        d_mixed = jnp.concatenate([jnp.where(half == 0, d_mixed, got), jnp.where(half == 0, got, d_mixed)])
        out_grads = out_grads[:, :128] + swap_half(out_grads[:, 128:].astype(bf16)).astype(f32)
    block_output = middle + scatter_near(act_later, down_rows) + bias_down
    d_queries, d_keys, d_values, sums = attn_bwd(queries, keys, values, d_mixed, mixed, log_total, min(512, tokens))
    d_qkv = jnp.concatenate([d_queries, d_keys, d_values], axis=1)
    d_normed_one = scatter(d_qkv, head_rows)
    d_input_norm, grad_gain_one, grad_shift_one = pull_one(d_normed_one)
    input_grad = d_middle + d_input_norm
    head_grads = dot(d_qkv, normed_one_all, ((0,), (0,)))
    if fast:
        gh = jnp.pad(head_grads.astype(bf16), ((0, 0), (0, WIDE - D))).reshape(48, 8, WIDE)
        got = collect(gh, out_grads.astype(bf16).reshape(D // 8, 8, 128), n_x, n_c, next(ids))
        attn_shard = (got[0].astype(f32) + got[1].astype(f32)).reshape(cols, WIDE)[:, :D].T
    else:
        room = jnp.zeros((3, n_c * 128, D), f32)
        room = lax.dynamic_update_slice_in_dim(room, head_grads.reshape(3, 128, D), ctx * 128, 1)[:, :D].reshape(3 * D, D)
        room_out = lax.dynamic_update_slice_in_dim(jnp.zeros((D, n_c * 128), f32), out_grads, ctx * 128, 1)[:, :D]
        attn_shard = lax.psum_scatter(jnp.concatenate([room, room_out]), both, scatter_dimension=0, tiled=True).T

    def placed(part):
        return lax.dynamic_update_slice_in_dim(jnp.zeros((n_c * 128,), f32), part, ctx * 128, 0)[:D]

    d_pre_sum = jnp.sum(d_pre, axis=0)
    up_grads = jnp.zeros((4 * D,), f32)
    for i, first in enumerate(up_first):
        up_grads = lax.dynamic_update_slice_in_dim(up_grads, d_pre_sum[i * cols : (i + 1) * cols], first - 8 * D, 0)
    grad_vectors = jnp.concatenate(
        [
            grad_gain_one,
            grad_shift_one,
            placed(sums[0]),
            placed(sums[1]),
            jnp.sum(d_middle, axis=0),
            grad_gain_two,
            grad_shift_two,
            jnp.sum(grad_output, axis=0),
            up_grads,
        ]
    )
    if fast:
        parts = jnp.pad(grad_vectors.reshape(n, owned), ((0, 0), (0, 1024 - owned))).reshape(n, 8, 128)
        vector_shard = reduce_vectors(parts, n_x, n_c, next(ids)).reshape(-1)[:owned]
    else:
        vector_shard = lax.psum_scatter(grad_vectors, both, scatter_dimension=0, tiled=True)
    return (block_output[None], input_grad[None], attn_shard, fc_shard, down_shard, vector_shard)


def solution(mesh):
    tokens_spec = P("fsdp", "ctx", None)
    cols_spec = P(None, ("fsdp", "ctx"))
    vec_spec = P(("fsdp", "ctx"))
    return jax.shard_map(
        per_device,
        mesh=mesh,
        in_specs=(tokens_spec, cols_spec, cols_spec, cols_spec, vec_spec, tokens_spec),
        out_specs=(tokens_spec, tokens_spec, cols_spec, cols_spec, cols_spec, vec_spec),
        check_vma=False,
    )
```
